32 devices in a mesh: ep: 8 (over z, x), dp: 4 (over y, core).
Axes of the slice: x: 2, y: 2, z: 4, core: 2. Of those that a mesh axis runs over, the one named last changes fastest.
Arguments:
- residual: bfloat16 [4096, 2880], P(('ep', 'dp')), may hold values from -400 to 400, as said below
- norm_gain: float32 [2880], replicated, may hold values from 0.25 to 1.75
- router_weight: bfloat16 [2880, 32], replicated, may hold values from -0.109375 to 0.109375
- out_grad: bfloat16 [4096, 2880], P(('ep', 'dp')), may hold values from -6 to 6
- expert_ids: int32 [4096, 4], P(('ep', 'dp')), may hold values from 0 to 31, all different within a row; in each aligned block of 128 rows (0 to 127, 128 to 255, ...) at most 24 rows name the same one
- hidden: bfloat16 [32, 768, 1440], P(('ep', 'dp')), may hold values from -0.3125 to 0.3125
- down_weight: bfloat16 [32, 1440, 2880], P(('ep', 'dp')), may hold values from -0.15625 to 0.15625
Outputs:
- hidden_grad: bfloat16 [32, 768, 1440], P(('ep', 'dp'))
- down_weight_grad: bfloat16 [32, 1440, 2880], P(('ep', 'dp'))
- residual_grad: bfloat16 [4096, 2880], P(('ep', 'dp'))
- router_grad: float32 [2880, 32], replicated
- gain_grad: float32 [2880], replicated
The draws below stay inside these ranges and needn't reach their ends.
Inputs may be any that keep to these rules, and one draw needn't show every extreme that they name: `expert_ids`: in the tokens of one device no expert is named more than 24 times, a bound that some block reaches. `residual`: Real-valued entries.
All inputs are finite; a program needn't handle non-finite values.
Results may differ from the reference program's by a relative error of at most 0.0085.
Values may be sent and summed in bfloat16 or wider, within the bound.
A program may use at most 128 MiB of HBM per device.

```python
import math
import jax
import jax.numpy as jnp
import numpy as np
from jax import lax

D = 2880
TOPK = 4
FF = 1440
TOK_DEV = 128
EXPERTS = 32
TOKENS = 4096
CAP = 24
SLOTS = 768
N_EP = 8
N_DP = 4


def draw_residual(key, part):
    key_rows, key_cols, key_base = jax.random.split(key, 3)
    row_scale = jnp.exp(jax.random.uniform(key_rows, (TOKENS, 1), jnp.float32, 0.0, math.log(10.0)))
    column_scale = jnp.exp(jax.random.uniform(key_cols, (1, D), jnp.float32, 0.0, math.log(10.0)))
    base = jax.random.truncated_normal(key_base, -3.5, 3.5, (TOKENS, D), jnp.float32)
    return (base * row_scale * column_scale).astype(jnp.bfloat16)


def shard_levels(own_key, dims, pieces, least, high):
    loudness = 1.0
    for dim, shards_of in pieces:
        draws = jax.random.uniform(jax.random.fold_in(jax.random.fold_in(own_key, 6), dim), (shards_of,), jnp.float32, least / len(pieces), high / len(pieces))
        loudness = loudness * jnp.repeat(jnp.exp(draws), dims[dim] // shards_of).reshape((-1,) + (1,) * (len(dims) - 1 - dim))
    return loudness


def deal_out(key, own, number, rows, number_of, top, reach, skew):
    sequence = jax.random.permutation(key, number_of)
    crowded, ordinary = load_shares(number_of, rows * top, reach, skew, True), load_shares(number_of, rows * top, reach, skew, False)
    places = jnp.arange(number_of)

    def named(tallies, turn):
        used = int((tallies > 0).sum())
        fixed = max(1, used // 4)
        passed = fixed + (places - fixed + turn * (used - fixed)) % max(1, number_of - fixed)
        return jnp.zeros((number_of,), jnp.int32).at[sequence[jnp.where(places < fixed, places, passed)]].set(jnp.asarray(tallies, jnp.int32))

    tallies = jnp.where(number % 4 == 0, named(crowded, number // 4), named(ordinary, number - number // 4 - 1))
    mixed = jax.random.permutation(jax.random.fold_in(own, 3), number_of)
    source_of, sink = mixed[0:number_of // 2 * 2:2], mixed[1:number_of // 2 * 2:2]
    slack = jnp.minimum(tallies[source_of] - 1, reach - tallies[sink]) // 2
    slack = jnp.where((source_of == sequence[0]) | (sink == sequence[0]) | (tallies[sink] == 0), 0, jnp.maximum(slack, 0))
    passed = jax.random.randint(jax.random.fold_in(own, 4), (number_of // 2,), 0, 1 << 20) % (slack + 1)
    tallies = tallies.at[source_of].add(-passed).at[sink].add(passed)
    items = jnp.searchsorted(jnp.cumsum(tallies), jnp.arange(rows * top), side="right").astype(jnp.int32)
    grid = items.reshape(top, rows).T
    grid = grid[jax.random.permutation(jax.random.fold_in(own, 1), rows)]
    turn = jax.random.randint(jax.random.fold_in(own, 2), (rows, 1), 0, top)
    return jnp.take_along_axis(grid, (jnp.arange(top)[None, :] + turn) % top, axis=1)


def load_shares(count, total, reach, slope, full):
    weights = [(1 << 20) // math.isqrt(standing ** slope) + 1 for standing in range(1, count + 1)]
    largest = reach if full else min(reach, max(-(-total // count), total * weights[0] // sum(weights)))
    least = 1 if total - largest >= count - 1 else 0
    given, rest = [largest] + [least] * (count - 1), total - largest - least * (count - 1)
    while rest > 0:
        free = [i for i in range(1, count) if given[i] < largest] or [i for i in range(1, count) if given[i] < reach]
        mass, remaining = sum([weights[i] for i in free]), rest
        for i in free:
            addition = min(reach - given[i], max(1, remaining * weights[i] // mass), rest)
            given[i] = given[i] + addition
            rest = rest - addition
    return np.array(given)


def scatter_about(rng, shape, scale, limit, shards=(), held_as=jnp.bfloat16):
    level = shard_levels(rng, shape, shards, -0.22, 0.18) if shards else 1.0
    values = jax.random.normal(rng, shape, jnp.float32) * scale * level
    return jnp.minimum(jnp.maximum(values, -limit), limit).astype(held_as)


def setup_inputs(seed: int = 0) -> dict:
    streams_of = jax.random.split(jax.random.key(seed), 8)
    residual = draw_residual(jax.random.fold_in(streams_of[7], 71), 0)
    norm_gain = jnp.clip(1.0 + 0.15 * jax.random.normal(streams_of[1], (D,), jnp.float32), 0.25, 1.75)
    router_weight = scatter_about(streams_of[2], (D, EXPERTS), D ** -0.5, 0.109375)
    out_grad = scatter_about(streams_of[3], (TOKENS, D), 1.0, 6.0, ((0, 32),))
    expert_ids_keys = jax.random.split(jax.random.fold_in(streams_of[4], 1), TOKENS // TOK_DEV)
    expert_ids_turns = jax.random.permutation(jax.random.fold_in(streams_of[4], 3), TOKENS // TOK_DEV)
    expert_ids = jax.vmap(lambda own, number: deal_out(jax.random.fold_in(streams_of[4], 2), own, number, TOK_DEV, EXPERTS, TOPK, CAP, 2))(expert_ids_keys, expert_ids_turns).reshape((TOKENS, TOPK))
    hidden = scatter_about(streams_of[5], (EXPERTS, SLOTS, FF), 0.05, 0.3125, ((0, 32),))
    down_weight = scatter_about(streams_of[6], (EXPERTS, FF, D), FF ** -0.5, 0.15625, ((0, 32),))
    return {"residual": residual, "norm_gain": norm_gain, "router_weight": router_weight, "out_grad": out_grad, "expert_ids": expert_ids, "hidden": hidden, "down_weight": down_weight}


def expert_step(packed):
    sent_grad, sent_prob, hidden_rows, weight = packed
    inner = lax.dot_general(sent_grad, weight, (((1,), (1,)), ((), ())), preferred_element_type=jnp.float32)
    slot_score = lax.optimization_barrier(jnp.sum(inner * hidden_rows.astype(jnp.float32), -1))
    weight_col = sent_prob.astype(jnp.float32)[:, None]
    hidden_grad = (weight_col * inner).astype(jnp.bfloat16)
    scaled = (weight_col * sent_grad.astype(jnp.float32)).astype(jnp.bfloat16)
    weight_grad = lax.dot_general(hidden_rows, scaled, (((0,), (0,)), ((), ())), preferred_element_type=jnp.float32)
    return (slot_score, hidden_grad, weight_grad.astype(jnp.bfloat16))

def reference(residual, norm_gain, router_weight, out_grad, expert_ids, hidden, down_weight):
    sources = N_EP * N_DP
    floated = residual.astype(jnp.float32)
    inverse = lax.rsqrt(lax.optimization_barrier(jnp.mean(floated * floated, -1, keepdims=True)) + 1e-05)
    unit = floated * inverse
    normed = (unit * norm_gain).astype(jnp.bfloat16)
    logits = jnp.dot(normed, router_weight, preferred_element_type=jnp.float32)
    picked = jnp.take_along_axis(logits, expert_ids, 1)
    expo = jnp.exp(picked)
    prob = expo / lax.optimization_barrier(jnp.sum(expo, -1, keepdims=True))
    flat_ids = expert_ids.reshape(sources, TOK_DEV * TOPK)
    onehot = (flat_ids[:, :, None] == jnp.arange(EXPERTS, dtype=jnp.int32)[None, None, :]).astype(jnp.int32)
    before = jnp.cumsum(onehot, 1) - onehot
    slot_rank = lax.optimization_barrier(jnp.sum(before * onehot, -1))
    source_idx = jnp.arange(sources, dtype=jnp.int32)[:, None]
    place = (flat_ids * SLOTS + source_idx * CAP + slot_rank).reshape(-1).astype(jnp.int32)
    repeated = jnp.repeat(out_grad, TOPK, axis=0)
    sent_grad = jnp.zeros((EXPERTS * SLOTS, D), jnp.bfloat16).at[place].set(repeated).reshape(EXPERTS, SLOTS, D)
    sent_prob = jnp.zeros((EXPERTS * SLOTS,), jnp.bfloat16).at[place].set(prob.astype(jnp.bfloat16).reshape(-1)).reshape(EXPERTS, SLOTS)
    slot_score, hidden_grad, down_weight_grad = lax.map(expert_step, (sent_grad, sent_prob, hidden, down_weight))
    score = slot_score.reshape(-1)[place].reshape(TOKENS, TOPK)
    pick_grad = prob * (score - lax.optimization_barrier(jnp.sum(prob * score, -1, keepdims=True)))
    match = expert_ids[:, :, None] == jnp.arange(EXPERTS, dtype=jnp.int32)[None, None, :]
    logit_grad = lax.optimization_barrier(jnp.sum(jnp.where(match, pick_grad[:, :, None], jnp.float32(0.0)), 1))
    router_grad = jnp.dot(normed.astype(jnp.float32).T, logit_grad, precision=lax.Precision.HIGHEST)
    normed_grad = jnp.dot(logit_grad, router_weight.astype(jnp.float32).T, precision=lax.Precision.HIGHEST)
    gain_grad = lax.optimization_barrier(jnp.sum(normed_grad * unit, 0))
    upper = normed_grad * norm_gain
    residual_grad = (inverse * (upper - unit * lax.optimization_barrier(jnp.mean(upper * unit, -1, keepdims=True)))).astype(jnp.bfloat16)
    return (hidden_grad, down_weight_grad, residual_grad, router_grad, gain_grad)
```

```python
import functools

import jax
import jax.numpy as jnp
from jax import lax
from jax.experimental import pallas as pl
from jax.experimental.pallas import tpu as pltpu
from jax.sharding import PartitionSpec as P

F32 = jnp.float32
BF16 = jnp.bfloat16


def kernel(
    n_ep, n_dp, cap,
    res_ref, gain_ref, rwt_ref, og_ref, ids_ref, hid_any, w_any,
    hg_any, wg_any, rg_ref, rgt_ref, gg_ref,
    send, recv, w, hid, hidt, scaled, hg, wg, normed_s, unit_s, inv_s, prob_s, rank_s, rankt_s, probt_s,
    ssend, srecv, part, rsbuf, agbuf,
    in_sem, row_send, row_recv, sc_send, sc_recv, rs_send, rs_recv, ag_send, ag_recv, hg_sem, wg_sem,
):
    n = n_ep * n_dp
    tokens, width = res_ref.shape
    experts = rwt_ref.shape[0]
    ff = w.shape[0]
    pad_width = send.shape[2]
    group = n_dp * cap
    ep = lax.axis_index("ep")
    dp = lax.axis_index("dp")
    me = ep * n_dp + dp

    def remote(src, dst, s_sem, r_sem, dev_ep, dev_dp):
        return pltpu.make_async_remote_copy(
            src_ref=src, dst_ref=dst, send_sem=s_sem, recv_sem=r_sem,
            device_id=(dev_ep, dev_dp), device_id_type=pl.DeviceIdType.MESH,
        )

    barrier = pltpu.get_barrier_semaphore()

    def greet(i, _):
        @pl.when(i != me)
        def _():
            pl.semaphore_signal(
                barrier, inc=1, device_id=(i // n_dp, i % n_dp), device_id_type=pl.DeviceIdType.MESH
            )
        return 0

    lax.fori_loop(0, n, greet, 0)
    load_h = pltpu.make_async_copy(hid_any, hid, in_sem.at[0])
    load_w = pltpu.make_async_copy(w_any, w, in_sem.at[1])
    load_h.start()
    load_w.start()

    floated = res_ref[...].astype(F32)
    inverse = lax.rsqrt(jnp.mean(floated * floated, -1, keepdims=True) + 1e-05)
    unit = floated * inverse
    normed = (unit * gain_ref[...]).astype(BF16)
    unit_s[...] = unit
    inv_s[...] = inverse
    normed_s[...] = normed
    logits = lax.dot_general(
        normed, rwt_ref[...], (((1,), (1,)), ((), ())), preferred_element_type=F32
    )
    lane_e = lax.broadcasted_iota(jnp.int32, (tokens, experts), 1)
    match = jnp.zeros((tokens, experts), F32)
    ids = ids_ref[...]
    for k in range(ids.shape[1]):
        match = match + jnp.where(ids[:, k : k + 1] == lane_e, F32(1.0), F32(0.0))
    expo = jnp.where(match > 0, jnp.exp(logits), F32(0.0))
    prob = expo / jnp.sum(expo, -1, keepdims=True)
    row_t = lax.broadcasted_iota(jnp.int32, (tokens, tokens), 0)
    col_t = lax.broadcasted_iota(jnp.int32, (tokens, tokens), 1)
    lower = jnp.where(col_t < row_t, F32(1.0), F32(0.0)).astype(BF16)
    rank = jnp.dot(lower, match.astype(BF16), preferred_element_type=F32)
    rank = jnp.where(match > 0, rank, F32(-1.0))
    prob_s[...] = prob
    rank_s[...] = rank
    rankt_s[...] = rank.T.reshape(experts, 1, tokens)
    probt_s[...] = prob.T.reshape(experts, 1, tokens)

    pl.semaphore_wait(barrier, n - 1)

    def pack(g, _):
        to = lax.rem(ep + n_ep - 1 - g, n_ep)
        first = to * n_dp
        rt = rankt_s[pl.ds(first, n_dp)]
        pt = probt_s[pl.ds(first, n_dp)]
        slot = lax.broadcasted_iota(jnp.int32, (n_dp, cap, tokens), 1).astype(F32)
        hit = slot == rt
        hot = jnp.where(hit, F32(1.0), F32(0.0)).reshape(group, tokens).astype(BF16)
        weight = jnp.sum(jnp.where(hit, pt, F32(0.0)), -1, keepdims=True)
        rows = jnp.dot(hot, og_ref[...], preferred_element_type=F32)
        send[pl.ds(first, n_dp), :, pl.ds(0, width)] = rows.reshape(n_dp, cap, width).astype(BF16)
        send[pl.ds(first, n_dp), :, pl.ds(width, pad_width - width)] = jnp.broadcast_to(
            weight, (n_dp, cap, pad_width - width)
        ).astype(BF16)
        for k in range(n_dp):
            j = lax.rem(dp + k, n_dp)
            e = first + j

            @pl.when(e != me)
            def _():
                remote(
                    send.at[e], recv.at[me], row_send.at[e], row_recv.at[me], to, j
                ).start()

            @pl.when(e == me)
            def _():
                recv[me] = send[me]
        return 0

    lax.fori_loop(0, n_ep, pack, 0)

    load_h.wait()
    hidt[...] = hid[...].T
    load_w.wait()

    def wait_rows(src_ep):
        for k in range(n_dp):
            s = src_ep * n_dp + k

            @pl.when(s != me)
            def _():
                remote(send.at[s], recv.at[s], row_send.at[s], row_recv.at[s], src_ep, k).wait_recv()

    def take(src_ep):
        got = recv[pl.ds(src_ep * n_dp, n_dp)].astype(F32)
        return got.reshape(group, pad_width)

    def chunk(c, _):
        sources = (
            lax.rem(ep + 1 + 2 * c, n_ep),
            lax.rem(ep + 2 + 2 * c, n_ep),
        )
        for s in sources:
            wait_rows(s)
        rows = jnp.concatenate([take(s) for s in sources], 0)
        starts = [pl.multiple_of(s * group, group) for s in sources]
        h = jnp.concatenate([hid[pl.ds(b, group)] for b in starts], 0).astype(F32)
        grad = rows[:, :width]
        weight = rows[:, width : width + 1]
        inner = lax.dot_general(
            grad.astype(BF16), w[...], (((1,), (1,)), ((), ())), preferred_element_type=F32
        )
        score = jnp.sum(inner * h, -1, keepdims=True).reshape(2 * n_dp, cap, 1)
        at_row = lax.broadcasted_iota(jnp.int32, (2 * n_dp, cap, 128), 1)
        at_lane = lax.broadcasted_iota(jnp.int32, (2 * n_dp, cap, 128), 2)
        score = jnp.sum(jnp.where(at_row == at_lane, score, F32(0.0)), 1, keepdims=True)
        for i, s in enumerate(sources):
            ssend[pl.ds(s * n_dp, n_dp)] = score[i * n_dp : (i + 1) * n_dp]
            for k in range(n_dp):
                d = s * n_dp + k

                @pl.when(d != me)
                def _():
                    remote(ssend.at[d], srecv.at[me], sc_send.at[d], sc_recv.at[me], s, k).start()

                @pl.when(d == me)
                def _():
                    srecv[me] = ssend[me]

        hgrad = (weight * inner).astype(BF16)
        scale = (weight * grad).astype(BF16)
        for i, s in enumerate(sources):
            hg[pl.ds(starts[i], group)] = hgrad[i * group : (i + 1) * group]
            scaled[pl.ds(starts[i], group)] = scale[i * group : (i + 1) * group]
            pltpu.make_async_copy(
                hg.at[pl.ds(starts[i], group)], hg_any.at[pl.ds(starts[i], group)], hg_sem.at[s]
            ).start()
        return 0

    lax.fori_loop(0, n_ep // 2, chunk, 0)

    blocks = wg_sem.shape[0]
    rows_of = ff // blocks

    def wg_block(b, _):
        at = pl.ds(pl.multiple_of(b * rows_of, rows_of), rows_of)
        wg[at] = jnp.dot(hidt[at], scaled[...], preferred_element_type=F32).astype(BF16)
        pltpu.make_async_copy(wg.at[at], wg_any.at[at], wg_sem.at[b]).start()
        return 0

    def others(fn):
        def step(i, _):
            @pl.when(i != me)
            def _():
                fn(i)
            return 0
        lax.fori_loop(0, n, step, 0)

    cut1, cut2 = blocks // 5, (3 * blocks) // 5
    lax.fori_loop(0, cut1, wg_block, 0)

    others(lambda i: remote(ssend.at[i], srecv.at[i], sc_send.at[i], sc_recv.at[i], i // n_dp, i % n_dp).wait_recv())
    back = srecv[...].reshape(n, 128).T
    rank = rank_s[...]
    prob = prob_s[...]
    score = jnp.zeros((tokens, experts), F32)
    for r in range(cap):
        score = score + jnp.where(rank == F32(r), back[r : r + 1, :], F32(0.0))
    lg = prob * (score - jnp.sum(prob * score, -1, keepdims=True))
    lgt = lg.T
    hit = lgt.astype(BF16)
    lot = (lgt - hit.astype(F32)).astype(BF16)
    both = jnp.dot(jnp.concatenate([hit, lot], 0), normed_s[...], preferred_element_type=F32)
    router = both[:experts] + both[experts:]
    for e in range(experts):
        part[e] = router[e : e + 1, :]
    rsbuf[me] = part[me]
    others(lambda i: remote(part.at[i], rsbuf.at[me], rs_send.at[i], rs_recv.at[me], i // n_dp, i % n_dp).start())

    lax.fori_loop(cut1, cut2, wg_block, 0)

    others(lambda i: remote(part.at[i], rsbuf.at[i], rs_send.at[i], rs_recv.at[i], i // n_dp, i % n_dp).wait_recv())
    agbuf[me] = jnp.sum(rsbuf[...], 0)
    others(lambda i: remote(agbuf.at[me], agbuf.at[me], ag_send.at[i], ag_recv.at[me], i // n_dp, i % n_dp).start())

    hi = lg.astype(BF16)
    lo = (lg - hi.astype(F32)).astype(BF16)
    rwt = rwt_ref[...]
    ngrad = jnp.dot(hi, rwt, preferred_element_type=F32) + jnp.dot(lo, rwt, preferred_element_type=F32)
    upper = ngrad * gain_ref[...]
    unit = unit_s[...]
    mean = jnp.mean(upper * unit, -1, keepdims=True)
    rg_ref[...] = (inv_s[...] * (upper - unit * mean)).astype(BF16)

    lax.fori_loop(cut2, blocks, wg_block, 0)

    others(lambda i: remote(agbuf.at[me], agbuf.at[i], ag_send.at[i], ag_recv.at[i], i // n_dp, i % n_dp).wait_recv())
    total = agbuf[...].reshape(experts, width)
    rgt_ref[...] = total
    gg_ref[...] = jnp.sum(total * rwt.astype(F32), 0, keepdims=True) / gain_ref[...]

    def finish(i):
        remote(send.at[i], recv.at[me], row_send.at[i], row_recv.at[me], i // n_dp, i % n_dp).wait_send()
        remote(ssend.at[i], srecv.at[me], sc_send.at[i], sc_recv.at[me], i // n_dp, i % n_dp).wait_send()
        remote(part.at[i], rsbuf.at[me], rs_send.at[i], rs_recv.at[me], i // n_dp, i % n_dp).wait_send()
        remote(agbuf.at[me], agbuf.at[me], ag_send.at[i], ag_recv.at[me], i // n_dp, i % n_dp).wait_send()

    others(finish)

    def drain_h(g, _):
        at = pl.ds(pl.multiple_of(g * group, group), group)
        pltpu.make_async_copy(hg.at[at], hg_any.at[at], hg_sem.at[g]).wait()
        return 0

    lax.fori_loop(0, n_ep, drain_h, 0)

    def drain_w(b, _):
        at = pl.ds(pl.multiple_of(b * rows_of, rows_of), rows_of)
        pltpu.make_async_copy(wg.at[at], wg_any.at[at], wg_sem.at[b]).wait()
        return 0

    lax.fori_loop(0, blocks, drain_w, 0)


def on_device(n_ep, n_dp, residual, norm_gain, router_weight, out_grad, expert_ids, hidden, down_weight):
    n = n_ep * n_dp
    tokens, width = residual.shape
    experts = router_weight.shape[1]
    slots, ff = hidden.shape[1:]
    real_cap = slots // experts
    cap = -(-real_cap // 8) * 8
    pad_width = -(-(width + 1) // 128) * 128
    hid = hidden[0]
    if cap != real_cap:
        hid = jnp.pad(
            hid.reshape(experts, real_cap, ff), ((0, 0), (0, cap - real_cap), (0, 0))
        ).reshape(experts * cap, ff)
    rows = experts * cap
    blocks = max(b for b in range(1, 6) if ff % (b * 16) == 0)
    vmem = pl.BlockSpec(memory_space=pltpu.VMEM)
    anyspace = pl.BlockSpec(memory_space=pl.ANY)
    dma = pltpu.SemaphoreType.DMA
    hg, wg, rg, rgt, gg = pl.pallas_call(
        functools.partial(kernel, n_ep, n_dp, cap),
        out_shape=(
            jax.ShapeDtypeStruct((rows, ff), BF16),
            jax.ShapeDtypeStruct((ff, width), BF16),
            jax.ShapeDtypeStruct((tokens, width), BF16),
            jax.ShapeDtypeStruct((experts, width), F32),
            jax.ShapeDtypeStruct((1, width), F32),
        ),
        in_specs=[vmem] * 5 + [anyspace] * 2,
        out_specs=(anyspace, anyspace, vmem, vmem, vmem),
        scratch_shapes=[
            pltpu.VMEM((n, cap, pad_width), BF16),
            pltpu.VMEM((n, cap, pad_width), BF16),
            pltpu.VMEM((ff, width), BF16),
            pltpu.VMEM((rows, ff), BF16),
            pltpu.VMEM((ff, rows), BF16),
            pltpu.VMEM((rows, width), BF16),
            pltpu.VMEM((rows, ff), BF16),
            pltpu.VMEM((ff, width), BF16),
            pltpu.VMEM((tokens, width), BF16),
            pltpu.VMEM((tokens, width), F32),
            pltpu.VMEM((tokens, 1), F32),
            pltpu.VMEM((tokens, experts), F32),
            pltpu.VMEM((tokens, experts), F32),
            pltpu.VMEM((experts, 1, tokens), F32),
            pltpu.VMEM((experts, 1, tokens), F32),
            pltpu.VMEM((n, 1, 128), F32),
            pltpu.VMEM((n, 1, 128), F32),
            pltpu.VMEM((n, 1, width), F32),
            pltpu.VMEM((n, 1, width), F32),
            pltpu.VMEM((n, 1, width), F32),
            dma((2,)),
            dma((n,)), dma((n,)), dma((n,)), dma((n,)),
            dma((n,)), dma((n,)), dma((n,)), dma((n,)),
            dma((n_ep,)),
            dma((blocks,)),
        ],
        compiler_params=pltpu.CompilerParams(
            collective_id=0, has_side_effects=True, vmem_limit_bytes=60 * 1024 * 1024
        ),
        name="expert_backward",
    )(residual, norm_gain[None], router_weight.T, out_grad, expert_ids, hid, down_weight[0])
    if cap != real_cap:
        hg = hg.reshape(experts, cap, ff)[:, :real_cap].reshape(slots, ff)
    return hg[None], wg[None], rg, rgt.T, gg[0]


def solution(mesh):
    both = ("ep", "dp")
    return jax.shard_map(
        functools.partial(on_device, mesh.shape["ep"], mesh.shape["dp"]),
        mesh=mesh,
        in_specs=(P(both, None), P(), P(), P(both, None), P(both, None), P(both, None, None), P(both, None, None)),
        out_specs=(P(both, None, None), P(both, None, None), P(both, None), P(), P()),
        check_vma=False,
    )
```

```python
import functools
import math

import jax
import jax.numpy as jnp
from jax import lax
from jax.experimental import pallas as pl
from jax.experimental.pallas import tpu as pltpu
from jax.sharding import PartitionSpec as P

F32 = jnp.float32
BF16 = jnp.bfloat16
LINE = 4


def kernel(
    n_ep, n_dp, lines, cap,
    res_ref, gain_ref, rwt_ref, og_ref, ids_ref, hid_any, w_any,
    hg_any, wg_any, rg_ref, rgt_ref, gg_ref,
    tok, meta, metat, send, recv, w, hid, hidt, scaled, hg, wg, normed_s, unit_s, inv_s, prob_s, rank_s,
    ssend, srecv, part, rsbuf, agbuf,
    in_sem, tok_send, tok_recv, meta_send, meta_recv, row_send, row_recv, sc_send, sc_recv, rs_send, rs_recv, ag_send, ag_recv, hg_sem, wg_sem,
):
    n = n_ep * n_dp
    tokens, width = res_ref.shape
    experts = rwt_ref.shape[0]
    ff = w.shape[0]
    pad_width = send.shape[2]
    plane = n // lines
    group = plane * cap
    me = lax.axis_index("ep") * n_dp + lax.axis_index("dp")
    z = me // plane
    p = me % plane

    def remote(src, dst, s_sem, r_sem, dev_ep, dev_dp):
        return pltpu.make_async_remote_copy(
            src_ref=src, dst_ref=dst, send_sem=s_sem, recv_sem=r_sem,
            device_id=(dev_ep, dev_dp), device_id_type=pl.DeviceIdType.MESH,
        )

    barrier = pltpu.get_barrier_semaphore()

    def greet(i, _):
        @pl.when(i != me)
        def _():
            pl.semaphore_signal(
                barrier, inc=1, device_id=(i // n_dp, i % n_dp), device_id_type=pl.DeviceIdType.MESH
            )
        return 0

    lax.fori_loop(0, n, greet, 0)
    load_h = pltpu.make_async_copy(hid_any, hid, in_sem.at[0])
    load_w = pltpu.make_async_copy(w_any, w, in_sem.at[1])
    load_h.start()
    load_w.start()

    floated = res_ref[...].astype(F32)
    inverse = lax.rsqrt(jnp.mean(floated * floated, -1, keepdims=True) + 1e-05)
    unit = floated * inverse
    normed = (unit * gain_ref[...]).astype(BF16)
    unit_s[...] = unit
    inv_s[...] = inverse
    normed_s[...] = normed
    logits = lax.dot_general(
        normed, rwt_ref[...], (((1,), (1,)), ((), ())), preferred_element_type=F32
    )
    lane_e = lax.broadcasted_iota(jnp.int32, (tokens, experts), 1)
    match = jnp.zeros((tokens, experts), F32)
    ids = ids_ref[...]
    for k in range(ids.shape[1]):
        match = match + jnp.where(ids[:, k : k + 1] == lane_e, F32(1.0), F32(0.0))
    expo = jnp.where(match > 0, jnp.exp(logits), F32(0.0))
    prob = expo / jnp.sum(expo, -1, keepdims=True)
    row_t = lax.broadcasted_iota(jnp.int32, (tokens, tokens), 0)
    col_t = lax.broadcasted_iota(jnp.int32, (tokens, tokens), 1)
    lower = jnp.where(col_t < row_t, F32(1.0), F32(0.0)).astype(BF16)
    rank = jnp.dot(lower, match.astype(BF16), preferred_element_type=F32)
    rank = jnp.where(match > 0, rank, F32(-1.0))
    prob_s[...] = prob
    rank_s[...] = rank
    tok[z] = og_ref[...]
    meta[z] = jnp.concatenate([rank.T, prob.T], 0).astype(BF16)

    pl.semaphore_wait(barrier, n - 1)

    def along(src, source, side):
        to = (z + 2 * side - 1) * plane + p
        return (
            remote(src, tok.at[source], tok_send.at[source, side], tok_recv.at[source], to // n_dp, to % n_dp),
            remote(
                meta.at[source], meta.at[source], meta_send.at[source, side], meta_recv.at[source],
                to // n_dp, to % n_dp,
            ),
        )

    def start_along(src, source, side):
        nxt = z + 2 * side - 1

        @pl.when((nxt >= 0) & (nxt < lines))
        def _():
            for c in along(src, source, side):
                c.start()

    start_along(og_ref, z, 0)
    start_along(og_ref, z, 1)

    def sides(k, fn):
        def step(i, _):
            source = z + k * (2 * i - 1)

            @pl.when((source >= 0) & (source < lines) & (k + 1 - i > 0) & (k >= 0))
            def _():
                fn(source, i)
            return 0
        lax.fori_loop(0, 2, step, 0)

    def forward(source, i):
        for c in along(tok.at[source], source, i):
            c.wait_recv()
        start_along(tok.at[source], source, 1 - i)

    def pack(source, _):
        metat[...] = meta[source].astype(F32).reshape(2 * experts, 1, tokens)
        rt = metat[pl.ds(z * plane, plane)]
        pt = metat[pl.ds(experts + z * plane, plane)]
        slot = lax.broadcasted_iota(jnp.int32, (plane, cap, tokens), 1).astype(F32)
        hit = slot == rt
        hot = jnp.where(hit, F32(1.0), F32(0.0)).reshape(group, tokens).astype(BF16)
        weight = jnp.sum(jnp.where(hit, pt, F32(0.0)), -1, keepdims=True)
        rows = jnp.dot(hot, tok[source], preferred_element_type=F32)
        first = source * plane
        send[pl.ds(first, plane), :, pl.ds(0, width)] = rows.reshape(plane, cap, width).astype(BF16)
        send[pl.ds(first, plane), :, pl.ds(width, pad_width - width)] = jnp.broadcast_to(
            weight, (plane, cap, pad_width - width)
        ).astype(BF16)
        own = first + p
        recv[own] = send[own]

        def push(k, _):
            q = (p + k) % plane
            row_copy(first, z * plane + q, q).start()
            return 0

        lax.fori_loop(1, plane, push, 0)

    def row_copy(first, to, q):
        return remote(
            send.at[first + q], recv.at[first + p], row_send.at[first + q], row_recv.at[first + p],
            to // n_dp, to % n_dp,
        )

    def wait_row(first, q):
        to = z * plane + q
        return remote(
            send.at[first + q], recv.at[first + q], row_send.at[first + q], row_recv.at[first + q],
            to // n_dp, to % n_dp,
        )

    def chunk(source, _):
        first = source * plane

        def arrive(k, _):
            wait_row(first, (p + k) % plane).wait_recv()
            return 0

        lax.fori_loop(1, plane, arrive, 0)
        rows = recv[pl.ds(first, plane)].astype(F32).reshape(group, pad_width)
        at = pl.ds(pl.multiple_of(first * cap, group), group)
        h = hid[at].astype(F32)
        grad = rows[:, :width]
        weight = rows[:, width : width + 1]
        inner = lax.dot_general(
            grad.astype(BF16), w[...], (((1,), (1,)), ((), ())), preferred_element_type=F32
        )
        score = jnp.sum(inner * h, -1, keepdims=True).reshape(plane, cap, 1)
        at_row = lax.broadcasted_iota(jnp.int32, (plane, cap, 128), 1)
        at_lane = lax.broadcasted_iota(jnp.int32, (plane, cap, 128), 2)
        ssend[pl.ds(first, plane)] = jnp.sum(
            jnp.where(at_row == at_lane, score, F32(0.0)), 1, keepdims=True
        )

        def push(k, _):
            d = first + k

            @pl.when(d != me)
            def _():
                remote(
                    ssend.at[d], srecv.at[me], sc_send.at[d], sc_recv.at[me], d // n_dp, d % n_dp
                ).start()
            return 0

        lax.fori_loop(0, plane, push, 0)

        @pl.when(source == z)
        def _():
            srecv[me] = ssend[me]

        hg[at] = (weight * inner).astype(BF16)
        scaled[at] = (weight * grad).astype(BF16)
        pltpu.make_async_copy(hg.at[at], hg_any.at[at], hg_sem.at[source]).start()

    def stage(k, _):
        @pl.when((k > 0) & (k < lines))
        def _():
            sides(k, forward)

        @pl.when(k < lines)
        def _():
            sides(k, pack)

        @pl.when(k == 0)
        def _():
            load_h.wait()
            hidt[...] = hid[...].T
            load_w.wait()

        sides(k - 1, chunk)
        return 0

    lax.fori_loop(0, lines + 1, stage, 0)

    blocks = wg_sem.shape[0]
    rows_of = ff // blocks

    def wg_block(b, _):
        at = pl.ds(pl.multiple_of(b * rows_of, rows_of), rows_of)
        wg[at] = jnp.dot(hidt[at], scaled[...], preferred_element_type=F32).astype(BF16)
        pltpu.make_async_copy(wg.at[at], wg_any.at[at], wg_sem.at[b]).start()
        return 0

    def others(fn):
        def step(i, _):
            @pl.when(i != me)
            def _():
                fn(i)
            return 0
        lax.fori_loop(0, n, step, 0)

    cut1, cut2 = blocks // 5, (3 * blocks) // 5
    lax.fori_loop(0, cut1, wg_block, 0)

    others(lambda i: remote(ssend.at[i], srecv.at[i], sc_send.at[i], sc_recv.at[i], i // n_dp, i % n_dp).wait_recv())
    back = srecv[...].reshape(n, 128).T
    rank = rank_s[...]
    prob = prob_s[...]
    score = jnp.zeros((tokens, experts), F32)
    for r in range(cap):
        score = score + jnp.where(rank == F32(r), back[r : r + 1, :], F32(0.0))
    lg = prob * (score - jnp.sum(prob * score, -1, keepdims=True))
    lgt = lg.T
    hit = lgt.astype(BF16)
    lot = (lgt - hit.astype(F32)).astype(BF16)
    both = jnp.dot(jnp.concatenate([hit, lot], 0), normed_s[...], preferred_element_type=F32)
    router = both[:experts] + both[experts:]
    for e in range(experts):
        part[e] = router[e : e + 1, :]
    rsbuf[me] = part[me]
    others(lambda i: remote(part.at[i], rsbuf.at[me], rs_send.at[i], rs_recv.at[me], i // n_dp, i % n_dp).start())

    lax.fori_loop(cut1, cut2, wg_block, 0)

    others(lambda i: remote(part.at[i], rsbuf.at[i], rs_send.at[i], rs_recv.at[i], i // n_dp, i % n_dp).wait_recv())
    agbuf[me] = jnp.sum(rsbuf[...], 0)
    others(lambda i: remote(agbuf.at[me], agbuf.at[me], ag_send.at[i], ag_recv.at[me], i // n_dp, i % n_dp).start())

    hi = lg.astype(BF16)
    lo = (lg - hi.astype(F32)).astype(BF16)
    rwt = rwt_ref[...]
    ngrad = jnp.dot(hi, rwt, preferred_element_type=F32) + jnp.dot(lo, rwt, preferred_element_type=F32)
    upper = ngrad * gain_ref[...]
    unit = unit_s[...]
    mean = jnp.mean(upper * unit, -1, keepdims=True)
    rg_ref[...] = (inv_s[...] * (upper - unit * mean)).astype(BF16)

    lax.fori_loop(cut2, blocks, wg_block, 0)

    others(lambda i: remote(agbuf.at[me], agbuf.at[i], ag_send.at[i], ag_recv.at[i], i // n_dp, i % n_dp).wait_recv())
    total = agbuf[...].reshape(experts, width)
    rgt_ref[...] = total
    gg_ref[...] = jnp.sum(total * rwt.astype(F32), 0, keepdims=True) / gain_ref[...]

    def finish(i):
        remote(ssend.at[i], srecv.at[me], sc_send.at[i], sc_recv.at[me], i // n_dp, i % n_dp).wait_send()
        remote(part.at[i], rsbuf.at[me], rs_send.at[i], rs_recv.at[me], i // n_dp, i % n_dp).wait_send()
        remote(agbuf.at[me], agbuf.at[me], ag_send.at[i], ag_recv.at[me], i // n_dp, i % n_dp).wait_send()

    others(finish)

    def finish_rows(source, _):
        def step(k, _):
            q = (p + k) % plane
            row_copy(source * plane, z * plane + q, q).wait_send()
            return 0
        lax.fori_loop(1, plane, step, 0)

        def sent(side):
            nxt = z + 2 * side - 1

            @pl.when((nxt >= 0) & (nxt < lines))
            def _():
                for c in along(tok.at[source], source, side):
                    c.wait_send()

        @pl.when(source <= z)
        def _():
            sent(1)

        @pl.when(source >= z)
        def _():
            sent(0)
        return 0

    lax.fori_loop(0, lines, finish_rows, 0)

    def drain_h(g, _):
        at = pl.ds(pl.multiple_of(g * group, group), group)
        pltpu.make_async_copy(hg.at[at], hg_any.at[at], hg_sem.at[g]).wait()
        return 0

    lax.fori_loop(0, lines, drain_h, 0)

    def drain_w(b, _):
        at = pl.ds(pl.multiple_of(b * rows_of, rows_of), rows_of)
        pltpu.make_async_copy(wg.at[at], wg_any.at[at], wg_sem.at[b]).wait()
        return 0

    lax.fori_loop(0, blocks, drain_w, 0)


def on_device(n_ep, n_dp, residual, norm_gain, router_weight, out_grad, expert_ids, hidden, down_weight):
    n = n_ep * n_dp
    lines = math.gcd(n_ep, LINE)
    tokens, width = residual.shape
    experts = router_weight.shape[1]
    slots, ff = hidden.shape[1:]
    real_cap = slots // experts
    cap = -(-real_cap // 8) * 8
    pad_width = -(-(width + 1) // 128) * 128
    hid = hidden[0]
    if cap != real_cap:
        hid = jnp.pad(
            hid.reshape(experts, real_cap, ff), ((0, 0), (0, cap - real_cap), (0, 0))
        ).reshape(experts * cap, ff)
    rows = experts * cap
    blocks = max(b for b in range(1, 6) if ff % (b * 16) == 0)
    vmem = pl.BlockSpec(memory_space=pltpu.VMEM)
    anyspace = pl.BlockSpec(memory_space=pl.ANY)
    dma = pltpu.SemaphoreType.DMA
    hg, wg, rg, rgt, gg = pl.pallas_call(
        functools.partial(kernel, n_ep, n_dp, lines, cap),
        out_shape=(
            jax.ShapeDtypeStruct((rows, ff), BF16),
            jax.ShapeDtypeStruct((ff, width), BF16),
            jax.ShapeDtypeStruct((tokens, width), BF16),
            jax.ShapeDtypeStruct((experts, width), F32),
            jax.ShapeDtypeStruct((1, width), F32),
        ),
        in_specs=[vmem] * 5 + [anyspace] * 2,
        out_specs=(anyspace, anyspace, vmem, vmem, vmem),
        scratch_shapes=[
            pltpu.VMEM((lines, tokens, width), BF16),
            pltpu.VMEM((lines, 2 * experts, tokens), BF16),
            pltpu.VMEM((2 * experts, 1, tokens), F32),
            pltpu.VMEM((n, cap, pad_width), BF16),
            pltpu.VMEM((n, cap, pad_width), BF16),
            pltpu.VMEM((ff, width), BF16),
            pltpu.VMEM((rows, ff), BF16),
            pltpu.VMEM((ff, rows), BF16),
            pltpu.VMEM((rows, width), BF16),
            pltpu.VMEM((rows, ff), BF16),
            pltpu.VMEM((ff, width), BF16),
            pltpu.VMEM((tokens, width), BF16),
            pltpu.VMEM((tokens, width), F32),
            pltpu.VMEM((tokens, 1), F32),
            pltpu.VMEM((tokens, experts), F32),
            pltpu.VMEM((tokens, experts), F32),
            pltpu.VMEM((n, 1, 128), F32),
            pltpu.VMEM((n, 1, 128), F32),
            pltpu.VMEM((n, 1, width), F32),
            pltpu.VMEM((n, 1, width), F32),
            pltpu.VMEM((n, 1, width), F32),
            dma((2,)),
            dma((lines, 2)), dma((lines,)), dma((lines, 2)), dma((lines,)),
            dma((n,)), dma((n,)), dma((n,)), dma((n,)),
            dma((n,)), dma((n,)), dma((n,)), dma((n,)),
            dma((lines,)),
            dma((blocks,)),
        ],
        compiler_params=pltpu.CompilerParams(
            collective_id=0, has_side_effects=True, vmem_limit_bytes=67_000_000
        ),
        name="expert_backward",
    )(residual, norm_gain[None], router_weight.T, out_grad, expert_ids, hid, down_weight[0])
    if cap != real_cap:
        hg = hg.reshape(experts, cap, ff)[:, :real_cap].reshape(slots, ff)
    return hg[None], wg[None], rg, rgt.T, gg[0]


def solution(mesh):
    both = ("ep", "dp")
    return jax.shard_map(
        functools.partial(on_device, mesh.shape["ep"], mesh.shape["dp"]),
        mesh=mesh,
        in_specs=(P(both, None), P(), P(), P(both, None), P(both, None), P(both, None, None), P(both, None, None)),
        out_specs=(P(both, None, None), P(both, None, None), P(both, None), P(), P()),
        check_vma=False,
    )
```

```python
import functools
import math

import jax
import jax.numpy as jnp
from jax import lax
from jax.experimental import pallas as pl
from jax.experimental.pallas import tpu as pltpu
from jax.sharding import PartitionSpec as P

F32 = jnp.float32
BF16 = jnp.bfloat16
LINE = 4


def kernel(
    n_ep, n_dp, lines, cap,
    res_ref, gain_ref, rwt_ref, og_ref, ids_ref, hidt_any, w_any,
    hgt_any, wg_any, rg_ref, rgt_ref, gg_ref,
    tok, meta, metat, send, recv, w, hid3, hidt, scaled, hg3, hgt, wg, normed_s, unit_s, inv_s, prob_s, rank_s,
    ssend, srecv, part, rsbuf, agbuf,
    in_sem, tok_send, tok_recv, meta_send, meta_recv, row_send, row_recv, sc_send, sc_recv, rs_send, rs_recv, ag_send, ag_recv, hg_sem, wg_sem,
):
    n = n_ep * n_dp
    width, tokens = res_ref.shape
    experts = rwt_ref.shape[0]
    ff = w.shape[0]
    pad_width = send.shape[2]
    plane = n // lines
    group = plane * cap
    me = lax.axis_index("ep") * n_dp + lax.axis_index("dp")
    z = me // plane
    p = me % plane

    def remote(src, dst, s_sem, r_sem, dev_ep, dev_dp):
        return pltpu.make_async_remote_copy(
            src_ref=src, dst_ref=dst, send_sem=s_sem, recv_sem=r_sem,
            device_id=(dev_ep, dev_dp), device_id_type=pl.DeviceIdType.MESH,
        )

    barrier = pltpu.get_barrier_semaphore()

    def greet(i, _):
        @pl.when(i != me)
        def _():
            pl.semaphore_signal(
                barrier, inc=1, device_id=(i // n_dp, i % n_dp), device_id_type=pl.DeviceIdType.MESH
            )
        return 0

    lax.fori_loop(0, n, greet, 0)
    load_h = pltpu.make_async_copy(hidt_any, hidt, in_sem.at[0])
    load_w = pltpu.make_async_copy(w_any, w, in_sem.at[1])
    load_h.start()
    load_w.start()

    gain = jnp.broadcast_to(gain_ref[...], (tokens, width)).T
    ssend[...] = jnp.zeros_like(ssend)
    floated = res_ref[...].astype(F32)
    inverse = lax.rsqrt(jnp.mean(floated * floated, 0, keepdims=True) + 1e-05)
    unit = floated * inverse
    normed = (unit * gain).astype(BF16)
    unit_s[...] = unit
    inv_s[...] = inverse
    normed_s[...] = normed
    logits = jnp.dot(rwt_ref[...], normed, preferred_element_type=F32)
    row_e = lax.broadcasted_iota(jnp.int32, (experts, tokens), 0)
    match = jnp.zeros((experts, tokens), F32)
    ids = ids_ref[...]
    for k in range(ids.shape[0]):
        match = match + jnp.where(ids[k : k + 1, :] == row_e, F32(1.0), F32(0.0))
    expo = jnp.where(match > 0, jnp.exp(logits), F32(0.0))
    prob = expo / jnp.sum(expo, 0, keepdims=True)
    row_t = lax.broadcasted_iota(jnp.int32, (tokens, tokens), 0)
    col_t = lax.broadcasted_iota(jnp.int32, (tokens, tokens), 1)
    before = jnp.where(row_t < col_t, F32(1.0), F32(0.0)).astype(BF16)
    rank = jnp.dot(match.astype(BF16), before, preferred_element_type=F32)
    rank = jnp.where(match > 0, rank, F32(-1.0))
    prob_s[...] = prob
    rank_s[...] = rank
    tok[z] = og_ref[...]
    meta[z] = jnp.concatenate([rank, prob], 0).astype(BF16)

    pl.semaphore_wait(barrier, n - 1)

    def along(src, source, side):
        to = (z + 2 * side - 1) * plane + p
        return (
            remote(src, tok.at[source], tok_send.at[source, side], tok_recv.at[source], to // n_dp, to % n_dp),
            remote(
                meta.at[source], meta.at[source], meta_send.at[source, side], meta_recv.at[source],
                to // n_dp, to % n_dp,
            ),
        )

    def start_along(src, source, side):
        nxt = z + 2 * side - 1

        @pl.when((nxt >= 0) & (nxt < lines))
        def _():
            for c in along(src, source, side):
                c.start()

    start_along(og_ref, z, 0)
    start_along(og_ref, z, 1)

    def sides(k, fn):
        def step(i, _):
            source = z + k * (2 * i - 1)

            @pl.when((source >= 0) & (source < lines) & (k + 1 - i > 0) & (k >= 0))
            def _():
                fn(source, i)
            return 0
        lax.fori_loop(0, 2, step, 0)

    def forward(source, i):
        for c in along(tok.at[source], source, i):
            c.wait_recv()
        start_along(tok.at[source], source, 1 - i)

    def pack(source, _):
        metat[...] = meta[source].astype(F32).reshape(2 * experts, 1, tokens)
        rt = metat[pl.ds(z * plane, plane)]
        pt = metat[pl.ds(experts + z * plane, plane)]
        slot = lax.broadcasted_iota(jnp.int32, (plane, cap, tokens), 1).astype(F32)
        hit = slot == rt
        hot = jnp.where(hit, F32(1.0), F32(0.0)).reshape(group, tokens).astype(BF16)
        weight = jnp.sum(jnp.where(hit, pt, F32(0.0)), -1, keepdims=True)
        rows = lax.dot_general(
            hot, tok[source], (((1,), (1,)), ((), ())), preferred_element_type=F32
        )
        first = source * plane
        send[pl.ds(first, plane), :, pl.ds(0, width)] = rows.reshape(plane, cap, width).astype(BF16)
        send[pl.ds(first, plane), :, pl.ds(width, pad_width - width)] = jnp.broadcast_to(
            weight, (plane, cap, pad_width - width)
        ).astype(BF16)
        own = first + p
        recv[own] = send[own]

        def push(k, _):
            q = (p + k) % plane
            row_copy(first, z * plane + q, q).start()
            return 0

        lax.fori_loop(1, plane, push, 0)

    def row_copy(first, to, q):
        return remote(
            send.at[first + q], recv.at[first + p], row_send.at[first + q], row_recv.at[first + p],
            to // n_dp, to % n_dp,
        )

    def wait_row(first, q):
        to = z * plane + q
        return remote(
            send.at[first + q], recv.at[first + q], row_send.at[first + q], row_recv.at[first + q],
            to // n_dp, to % n_dp,
        )

    def chunk(source, _):
        first = source * plane

        def arrive(k, _):
            wait_row(first, (p + k) % plane).wait_recv()
            return 0

        lax.fori_loop(1, plane, arrive, 0)
        rows = recv[pl.ds(first, plane)].astype(F32).reshape(group, pad_width)
        at = pl.ds(pl.multiple_of(first * cap, group), group)
        h = hid3[source].astype(F32)
        grad = rows[:, :width]
        weight = rows[:, width : width + 1]
        inner = lax.dot_general(
            w[...], grad.astype(BF16), (((1,), (1,)), ((), ())), preferred_element_type=F32
        )
        score = jnp.sum(inner * h, 0, keepdims=True)
        for k in range(plane):
            ssend[first + k, :, pl.ds(0, cap)] = score[:, k * cap : (k + 1) * cap]

        def push(k, _):
            d = first + k

            @pl.when(d != me)
            def _():
                remote(
                    ssend.at[d], srecv.at[me], sc_send.at[d], sc_recv.at[me], d // n_dp, d % n_dp
                ).start()
            return 0

        lax.fori_loop(0, plane, push, 0)

        @pl.when(source == z)
        def _():
            srecv[me] = ssend[me]

        across = jnp.broadcast_to(weight, (group, 128)).T[0:1, :]
        hg3[source] = (across * inner).astype(BF16)
        scaled[at] = (weight * grad).astype(BF16)

    def stage(k, _):
        @pl.when((k > 0) & (k < lines))
        def _():
            sides(k, forward)

        @pl.when(k < lines)
        def _():
            sides(k, pack)

        @pl.when(k == 0)
        def _():
            load_h.wait()
            for i in range(lines):
                hid3[i] = hidt[:, i * group : (i + 1) * group]
            load_w.wait()

        sides(k - 1, chunk)
        return 0

    lax.fori_loop(0, lines + 1, stage, 0)

    for i in range(lines):
        hgt[:, i * group : (i + 1) * group] = hg3[i]
    store_h = pltpu.make_async_copy(hgt, hgt_any, hg_sem)
    store_h.start()

    blocks = wg_sem.shape[0]
    rows_of = ff // blocks

    def wg_copy(b):
        at = pl.ds(pl.multiple_of(b * rows_of, rows_of), rows_of)
        return pltpu.make_async_copy(wg.at[b % 2], wg_any.at[at], wg_sem.at[b])

    def wg_block(b, _):
        @pl.when(b >= 2)
        def _():
            wg_copy(b - 2).wait()

        at = pl.ds(pl.multiple_of(b * rows_of, rows_of), rows_of)
        wg[b % 2] = jnp.dot(hidt[at], scaled[...], preferred_element_type=F32).astype(BF16)
        wg_copy(b).start()
        return 0

    def others(fn):
        def step(i, _):
            @pl.when(i != me)
            def _():
                fn(i)
            return 0
        lax.fori_loop(0, n, step, 0)

    cut1, cut2 = blocks // 5, (3 * blocks) // 5
    lax.fori_loop(0, cut1, wg_block, 0)

    others(lambda i: remote(ssend.at[i], srecv.at[i], sc_send.at[i], sc_recv.at[i], i // n_dp, i % n_dp).wait_recv())
    back = srecv[...].reshape(n, 128)
    rank = rank_s[...]
    prob = prob_s[...]
    score = jnp.zeros((experts, tokens), F32)
    for r in range(cap):
        score = score + jnp.where(rank == F32(r), back[:, r : r + 1], F32(0.0))
    lg = prob * (score - jnp.sum(prob * score, 0, keepdims=True))
    hi = lg.astype(BF16)
    lo = (lg - hi.astype(F32)).astype(BF16)
    both = lax.dot_general(
        jnp.concatenate([hi, lo], 0), normed_s[...], (((1,), (1,)), ((), ())),
        preferred_element_type=F32,
    )
    router = both[:experts] + both[experts:]
    for e in range(experts):
        part[e] = router[e : e + 1, :]
    rsbuf[me] = part[me]
    others(lambda i: remote(part.at[i], rsbuf.at[me], rs_send.at[i], rs_recv.at[me], i // n_dp, i % n_dp).start())

    lax.fori_loop(cut1, cut2, wg_block, 0)

    others(lambda i: remote(part.at[i], rsbuf.at[i], rs_send.at[i], rs_recv.at[i], i // n_dp, i % n_dp).wait_recv())
    agbuf[me] = jnp.sum(rsbuf[...], 0)
    others(lambda i: remote(agbuf.at[me], agbuf.at[me], ag_send.at[i], ag_recv.at[me], i // n_dp, i % n_dp).start())

    rwt = rwt_ref[...]
    ngrad = lax.dot_general(
        jnp.concatenate([rwt, rwt], 0), jnp.concatenate([hi, lo], 0), (((0,), (0,)), ((), ())),
        preferred_element_type=F32,
    )
    upper = ngrad * jnp.broadcast_to(gain_ref[...], (tokens, width)).T
    unit = unit_s[...]
    mean = jnp.mean(upper * unit, 0, keepdims=True)
    rg_ref[...] = (inv_s[...] * (upper - unit * mean)).astype(BF16)

    lax.fori_loop(cut2, blocks, wg_block, 0)

    others(lambda i: remote(agbuf.at[me], agbuf.at[i], ag_send.at[i], ag_recv.at[i], i // n_dp, i % n_dp).wait_recv())
    total = agbuf[...].reshape(experts, width)
    rgt_ref[...] = total
    gg_ref[...] = jnp.sum(total * rwt.astype(F32), 0, keepdims=True) / gain_ref[...]

    def finish(i):
        remote(ssend.at[i], srecv.at[me], sc_send.at[i], sc_recv.at[me], i // n_dp, i % n_dp).wait_send()
        remote(part.at[i], rsbuf.at[me], rs_send.at[i], rs_recv.at[me], i // n_dp, i % n_dp).wait_send()
        remote(agbuf.at[me], agbuf.at[me], ag_send.at[i], ag_recv.at[me], i // n_dp, i % n_dp).wait_send()

    others(finish)

    def finish_rows(source, _):
        def step(k, _):
            q = (p + k) % plane
            row_copy(source * plane, z * plane + q, q).wait_send()
            return 0
        lax.fori_loop(1, plane, step, 0)

        def sent(side):
            nxt = z + 2 * side - 1

            @pl.when((nxt >= 0) & (nxt < lines))
            def _():
                for c in along(tok.at[source], source, side):
                    c.wait_send()

        @pl.when(source <= z)
        def _():
            sent(1)

        @pl.when(source >= z)
        def _():
            sent(0)
        return 0

    lax.fori_loop(0, lines, finish_rows, 0)

    store_h.wait()
    for b in range(max(0, blocks - 2), blocks):
        wg_copy(b).wait()


def on_device(n_ep, n_dp, residual, norm_gain, router_weight, out_grad, expert_ids, hidden, down_weight):
    n = n_ep * n_dp
    lines = math.gcd(n_ep, LINE)
    tokens, width = residual.shape
    experts = router_weight.shape[1]
    slots, ff = hidden.shape[1:]
    real_cap = slots // experts
    cap = -(-real_cap // 8) * 8
    pad_width = -(-(width + 1) // 128) * 128
    hidt = hidden[0].T
    if cap != real_cap:
        hidt = jnp.pad(
            hidt.reshape(ff, experts, real_cap), ((0, 0), (0, 0), (0, cap - real_cap))
        ).reshape(ff, experts * cap)
    rows = experts * cap
    blocks = max(b for b in range(1, 6) if ff % (b * 16) == 0)
    vmem = pl.BlockSpec(memory_space=pltpu.VMEM)
    anyspace = pl.BlockSpec(memory_space=pl.ANY)
    dma = pltpu.SemaphoreType.DMA
    hgt, wg, rg, rgt, gg = pl.pallas_call(
        functools.partial(kernel, n_ep, n_dp, lines, cap),
        out_shape=(
            jax.ShapeDtypeStruct((ff, rows), BF16),
            jax.ShapeDtypeStruct((ff, width), BF16),
            jax.ShapeDtypeStruct((width, tokens), BF16),
            jax.ShapeDtypeStruct((experts, width), F32),
            jax.ShapeDtypeStruct((1, width), F32),
        ),
        in_specs=[vmem] * 5 + [anyspace] * 2,
        out_specs=(anyspace, anyspace, vmem, vmem, vmem),
        scratch_shapes=[
            pltpu.VMEM((lines, width, tokens), BF16),
            pltpu.VMEM((lines, 2 * experts, tokens), BF16),
            pltpu.VMEM((2 * experts, 1, tokens), F32),
            pltpu.VMEM((n, cap, pad_width), BF16),
            pltpu.VMEM((n, cap, pad_width), BF16),
            pltpu.VMEM((ff, width), BF16),
            pltpu.VMEM((lines, ff, rows // lines), BF16),
            pltpu.VMEM((ff, rows), BF16),
            pltpu.VMEM((rows, width), BF16),
            pltpu.VMEM((lines, ff, rows // lines), BF16),
            pltpu.VMEM((ff, rows), BF16),
            pltpu.VMEM((2, ff // blocks, width), BF16),
            pltpu.VMEM((width, tokens), BF16),
            pltpu.VMEM((width, tokens), F32),
            pltpu.VMEM((1, tokens), F32),
            pltpu.VMEM((experts, tokens), F32),
            pltpu.VMEM((experts, tokens), F32),
            pltpu.VMEM((n, 1, 128), F32),
            pltpu.VMEM((n, 1, 128), F32),
            pltpu.VMEM((n, 1, width), F32),
            pltpu.VMEM((n, 1, width), F32),
            pltpu.VMEM((n, 1, width), F32),
            dma((2,)),
            dma((lines, 2)), dma((lines,)), dma((lines, 2)), dma((lines,)),
            dma((n,)), dma((n,)), dma((n,)), dma((n,)),
            dma((n,)), dma((n,)), dma((n,)), dma((n,)),
            dma,
            dma((blocks,)),
        ],
        compiler_params=pltpu.CompilerParams(
            collective_id=0, has_side_effects=True, vmem_limit_bytes=67_000_000
        ),
        name="expert_backward",
    )(residual.T, norm_gain[None], router_weight.T, out_grad.T, expert_ids.T, hidt, down_weight[0])
    if cap != real_cap:
        hgt = hgt.reshape(ff, experts, cap)[:, :, :real_cap].reshape(ff, slots)
    return hgt.T[None], wg[None], rg.T, rgt.T, gg[0]


def solution(mesh):
    both = ("ep", "dp")
    return jax.shard_map(
        functools.partial(on_device, mesh.shape["ep"], mesh.shape["dp"]),
        mesh=mesh,
        in_specs=(P(both, None), P(), P(), P(both, None), P(both, None), P(both, None, None), P(both, None, None)),
        out_specs=(P(both, None, None), P(both, None, None), P(both, None), P(), P()),
        check_vma=False,
    )
```
